128 devices in a mesh: ep: 4 (over z), fsdp: 32 (over y, x, core).
Axes of the slice: x: 4, y: 4, z: 4, core: 2. Of those that a mesh axis runs over, the one named last changes fastest.
Arguments:
- train_gate: float32 [64, 2048, 1408], P('ep', 'fsdp'), may hold values from -0.25 to 0.25
- train_up: float32 [64, 2048, 1408], P('ep', 'fsdp'), may hold values from -0.25 to 0.25
- train_down: float32 [64, 1408, 2048], P('ep', None, 'fsdp'), may hold values from -0.3125 to 0.3125
- router_weight: float32 [2048, 64], P('fsdp', 'ep'), may hold values from -0.125 to 0.125
- router_gain: float32 [2048], P('fsdp'), may hold values from 0.25 to 1.75
Outputs:
- ready_gate: bfloat16 [64, 2048, 1408], P('ep', None, 'fsdp')
- ready_up: bfloat16 [64, 2048, 1408], P('ep', None, 'fsdp')
- ready_down: bfloat16 [64, 1408, 2048], P('ep', 'fsdp')
- scale_gate: float32 [64, 1408], P('ep', 'fsdp')
- scale_up: float32 [64, 1408], P('ep', 'fsdp')
- scale_down: float32 [64, 1408], P('ep', 'fsdp')
- serve_router: bfloat16 [2048, 64], replicated
The draws below stay inside these ranges and needn't reach their ends.
All inputs are finite; a program needn't handle non-finite values.
Results may differ from the reference program's by a relative error of at most 0.001.
Values may be sent and summed in bfloat16 or wider, within the bound.
No kernel may reach another device: no remote copies, remote signals or barrier semaphores. Data moves between devices by JAX's collectives and lax.ppermute only.
A program may use at most 192 MiB of HBM per device.

```python
import jax
import jax.numpy as jnp
from jax import lax

EXPERTS = 64
D_MODEL = 2048
D_EXPERT = 1408


def strengthened(drawn, own_key, source, target, shards_of, factor):
    owner, partner = [(jnp.arange(drawn.shape[axis_at]) // (drawn.shape[axis_at] // shards_of)).reshape([-1 if axis == axis_at else 1 for axis in range(drawn.ndim)]) for axis_at in (source, target)]
    chosen = jax.random.permutation(own_key, shards_of)[partner]
    strong = (owner == chosen) | (owner == (partner + shards_of // 2) % shards_of)
    return jnp.where(strong, factor * drawn, drawn)


def block_scale(rng, extent, cuts, smallest, largest):
    gain, own = 1.0, jax.random.fold_in(rng, 6)
    for axis_at, blocks in cuts:
        steps = jnp.exp(jax.random.uniform(jax.random.fold_in(own, axis_at), (blocks,), jnp.float32, smallest / len(cuts), largest / len(cuts)))
        gain = gain * jnp.repeat(steps, extent[axis_at] // blocks).reshape([-1 if axis == axis_at else 1 for axis in range(len(extent))])
    return gain


def normal_values(rng, extent, width, reach, pieces=(), dtype=jnp.bfloat16):
    loudness = block_scale(rng, extent, pieces, -0.22, 0.18) if pieces else 1.0
    result = jax.random.normal(rng, extent, jnp.float32) * width * loudness
    return jnp.minimum(jnp.maximum(result, -reach), reach).astype(dtype)


def bell_draw_with(own_key, dims, width, reach, shards, heavy, held_as=jnp.bfloat16):
    values = width * jax.random.normal(own_key, dims, jnp.float32)
    if shards:
        values = values * block_scale(own_key, dims, shards, -0.22, 0.18)
    return jnp.clip(strengthened(values, jax.random.fold_in(own_key, 3), *heavy), -reach, reach).astype(held_as)


def setup_inputs(seed: int = 0) -> dict:
    seeds = jax.random.split(jax.random.key(seed), 6)
    return {
        "train_gate": bell_draw_with(seeds[0], (EXPERTS, D_MODEL, D_EXPERT), D_MODEL ** -0.5, 0.25, ((0, 4), (1, 32)), (1, 2, 32, 2.75), jnp.float32),
        "train_up": bell_draw_with(seeds[1], (EXPERTS, D_MODEL, D_EXPERT), D_MODEL ** -0.5, 0.25, ((0, 4), (1, 32)), (1, 2, 32, 2.75), jnp.float32),
        "train_down": bell_draw_with(seeds[2], (EXPERTS, D_EXPERT, D_MODEL), D_EXPERT ** -0.5, 0.3125, ((0, 4), (2, 32)), (2, 1, 32, 2.75), jnp.float32),
        "router_weight": normal_values(seeds[3], (D_MODEL, EXPERTS), D_MODEL ** -0.5, 0.125, ((0, 32), (1, 4)), jnp.float32),
        "router_gain": jnp.clip(1.0 + 0.15 * jax.random.normal(seeds[4], (D_MODEL,), jnp.float32), 0.25, 1.75),
    }


def reference(train_gate, train_up, train_down, router_weight, router_gain):
    scale_gate = jnp.sqrt(lax.optimization_barrier(jnp.sum(train_gate * train_gate, axis=1)))
    ready_gate = (train_gate / jnp.expand_dims(scale_gate, 1)).astype(jnp.bfloat16)
    scale_up = jnp.sqrt(lax.optimization_barrier(jnp.sum(train_up * train_up, axis=1)))
    ready_up = (train_up / jnp.expand_dims(scale_up, 1)).astype(jnp.bfloat16)
    scale_down = jnp.sqrt(lax.optimization_barrier(jnp.sum(train_down * train_down, axis=2)))
    ready_down = (train_down / jnp.expand_dims(scale_down, 2)).astype(jnp.bfloat16)
    serve_router = (router_weight * router_gain[:, None]).astype(jnp.bfloat16)
    return (ready_gate, ready_up, ready_down, scale_gate, scale_up, scale_down, serve_router)
```

```python
import functools

import jax
import jax.numpy as jnp
from jax import lax
from jax.experimental import pallas as pl
from jax.experimental.pallas import tpu as pltpu
from jax.sharding import Mesh, PartitionSpec as P


POWER = 17
REACH = 180.0
FLOOR = 1e-37
LANES = 128
HALF = LANES // 2
STEP = 4
SIDE = 4
PLANE = ("y", "x", "core")
SHIFTS = (
    (1, 0), (3, 0), (0, 1), (0, 3), (1, 1), (3, 3), (1, 3), (3, 1),
    (2, 0), (0, 2), (2, 1), (2, 3), (1, 2), (3, 2), (2, 2),
)


def anywhere(count):
    return [pl.BlockSpec(memory_space=pl.ANY)] * count


def rows_at(start, size, unit):
    return pl.ds(pl.multiple_of(start, unit), size)


def landed(ref, sem):
    pltpu.make_async_copy(ref, ref, sem).wait()


def chip_at(dx, dy):
    y, x = lax.axis_index("y"), lax.axis_index("x")
    return lax.rem(y + dy, SIDE) * SIDE + lax.rem(x + dx, SIDE)


def behind(ahead, kernel):
    return lambda *refs: kernel(*refs[ahead:])


def encode_tiles(x, xin, stage, pay, sums, notes, sem_in, peers, tiles, after):
    depth, experts, _, _ = xin.shape
    half = experts // 2
    share = tiles * LANES // peers
    odd = lax.axis_index("core")

    def fetch(i):
        slot = lax.rem(i, depth)
        at = rows_at(i * LANES, LANES, LANES)
        pltpu.make_async_copy(x.at[:, :, at], xin.at[slot], sem_in.at[slot]).start()

    def first(i, carry):
        fetch(i)
        return carry

    lax.fori_loop(0, depth, first, 0)

    def tile_of(i, carry):
        slot = lax.rem(i, depth)
        landed(xin.at[slot], sem_in.at[slot])
        at = rows_at(i * LANES, LANES, LANES)
        for e in range(half):
            a, b = xin[slot, e + half * odd], xin[slot, e + half * (1 - odd)]
            sa = jnp.sum(a * a, 0, keepdims=True)
            sb = jnp.sum(b * b, 0, keepdims=True)
            sums[pl.ds(e, 1), at] = sa
            sums[pl.ds(e + half, 1), at] = sb
            a = a * (REACH * lax.rsqrt(jnp.maximum(sa, FLOOR)))
            b = b * (REACH * lax.rsqrt(jnp.maximum(sb, FLOOR)))
            v = jnp.concatenate([a, b], 0)
            v2 = v * v
            v4 = v2 * v2
            v8 = v4 * v4
            y = v8 * v8 * v
            stage[pl.ds(e, LANES, stride=half), :] = y.T
        pay[rows_at(i * LANES * half, LANES * half, LANES * half), :] = stage[...].astype(jnp.bfloat16)

        @pl.when(i + depth < tiles)
        def _():
            fetch(i + depth)

        after(i)
        return carry

    lax.fori_loop(0, tiles, tile_of, 0)
    total = sums[...]
    total = jnp.where(odd == 1, jnp.concatenate([total[half:], total[:half]], 0), total)
    high = total.astype(jnp.bfloat16).astype(jnp.float32)
    low = total - high
    gap = jnp.zeros((experts, HALF - share), jnp.float32)
    for d in range(peers):
        piece = slice(d * share, (d + 1) * share)
        notes[d] = jnp.concatenate([high[:, piece], gap, low[:, piece], gap], 1).astype(jnp.bfloat16)


def encode_scratch(peers, experts, rows, columns, depth):
    return [
        pltpu.VMEM((depth, experts, rows, LANES), jnp.float32),
        pltpu.VMEM((LANES * experts // 2, LANES), jnp.float32),
        pltpu.VMEM((columns * experts // 2, LANES), jnp.bfloat16),
        pltpu.VMEM((experts, columns), jnp.float32),
        pltpu.VMEM((peers, experts, LANES), jnp.bfloat16),
        pltpu.SemaphoreType.DMA((depth,)),
        pltpu.SemaphoreType.DMA,
        pltpu.SemaphoreType.DMA,
    ]


def encode_bulk_kernel(routed, peers, tiles, *refs):
    x, out = refs[0], refs[1 + 2 * routed]
    xin, stage, pay, sums, notes, sem_in, sem_pay, sem_note = refs[2 + 2 * routed : 10 + 2 * routed]
    experts = xin.shape[1]
    half = experts // 2
    share = tiles * LANES // peers
    block = share * half

    if routed:
        weight, gain = refs[1:3]
        router, sem_router = refs[10 + 2 * routed :]
        part = weight[...] * gain[...]
        part = jnp.where(lax.axis_index("core") == 1, jnp.concatenate([part[half:], part[:half]], 0), part)
        part = jnp.concatenate([part[:half], part[half:]], 1)
        part = jnp.concatenate([part, jnp.zeros_like(part)], 0).astype(jnp.bfloat16)
        for d in range(peers):
            router[d] = part
        pltpu.make_async_copy(router, out.at[:, pl.ds(block + experts, experts), :], sem_router).start()

    def after(tile):
        def send(d, inner):
            pltpu.make_async_copy(
                pay.at[rows_at(d * block, block, 16), :], out.at[d, pl.ds(0, block), :], sem_pay
            ).start()
            return inner

        lax.fori_loop(tile * LANES // share, (tile + 1) * LANES // share, send, 0)

    encode_tiles(x, xin, stage, pay, sums, notes, sem_in, peers, tiles, after)
    pltpu.make_async_copy(notes, out.at[:, pl.ds(block, experts), :], sem_note).start()
    landed(pay, sem_pay)
    landed(notes, sem_note)
    if routed:
        landed(router, sem_router)


def encode_bulk(x, small, ahead, peers, depth=8):
    experts, rows, columns = x.shape
    routed = len(small) // 2
    height = columns // peers * experts // 2 + experts * (1 + routed)
    return pl.pallas_call(
        behind(len(ahead), functools.partial(encode_bulk_kernel, routed, peers, columns // LANES)),
        in_specs=anywhere(len(ahead) + 1) + [pl.BlockSpec(memory_space=pltpu.VMEM)] * len(small),
        out_specs=pl.BlockSpec(memory_space=pl.ANY),
        out_shape=jax.ShapeDtypeStruct((peers, height, LANES), jnp.bfloat16),
        scratch_shapes=encode_scratch(peers, experts, rows, columns, depth)
        + [pltpu.VMEM((peers, experts, LANES), jnp.bfloat16), pltpu.SemaphoreType.DMA] * routed,
        name="encode_bulk",
    )(*ahead, x, *small)


def encode_head_kernel(peers, tiles, x, keep, give, *scratch):
    xin, stage, pay, sums, notes, sem_in, sem_pay, sem_note = scratch
    experts = xin.shape[1]
    block = tiles * LANES // peers * experts // 2
    core = lax.axis_index("core")
    encode_tiles(x, xin, stage, pay, sums, notes, sem_in, peers, tiles, lambda tile: None)
    for k, (dx, dy) in enumerate(((0, 0),) + SHIFTS):
        chip = chip_at(dx, dy)
        for out, which in ((give, 1 - core), (keep, core)):
            d = 2 * chip + which
            pltpu.make_async_copy(
                pay.at[rows_at(d * block, block, 16), :], out.at[k, pl.ds(0, block), :], sem_pay
            ).start()
            pltpu.make_async_copy(notes.at[d], out.at[k, pl.ds(block, experts), :], sem_note).start()
    landed(pay, sem_pay)
    landed(notes, sem_note)


def encode_head(x, ahead, peers, depth=8):
    experts, rows, columns = x.shape
    height = columns // peers * experts // 2 + experts
    return pl.pallas_call(
        behind(len(ahead), functools.partial(encode_head_kernel, peers, columns // LANES)),
        in_specs=anywhere(len(ahead) + 1),
        out_specs=anywhere(2),
        out_shape=[jax.ShapeDtypeStruct((len(SHIFTS) + 1, height, LANES), jnp.bfloat16)] * 2,
        scratch_shapes=encode_scratch(peers, experts, rows, columns, depth),
        name="encode_head",
    )(*ahead, x)


def pair_kernel(keep, got, *refs):
    outs, (held, sem_in, sem_out) = refs[: len(SHIFTS) + 1], refs[len(SHIFTS) + 1 :]
    for k, a in enumerate((keep, got)):
        pltpu.make_async_copy(a, held.at[k], sem_in.at[k]).start()
    for k in range(2):
        landed(held.at[k], sem_in.at[k])
    for i, out in enumerate(outs):
        pltpu.make_async_copy(held.at[:, i], out, sem_out).start()
    landed(held, sem_out)


def paired(keep, got):
    count, height, _ = keep.shape
    return pl.pallas_call(
        pair_kernel,
        in_specs=anywhere(2),
        out_specs=anywhere(count),
        out_shape=[jax.ShapeDtypeStruct((2, height, LANES), jnp.bfloat16)] * count,
        scratch_shapes=[
            pltpu.VMEM((2, count, height, LANES), jnp.bfloat16),
            pltpu.SemaphoreType.DMA((2,)),
            pltpu.SemaphoreType.DMA,
        ],
        name="paired",
    )(keep, got)


def two_cores(a, b):
    left = lax.broadcasted_iota(jnp.int32, a.shape, 1) < HALF
    return jnp.concatenate([jnp.where(left, a, b), pltpu.roll(jnp.where(left, b, a), HALF, 1)], 0)


def decode_kernel(share, depth, head, routed, *refs):
    sources, refs = refs[:head] if head else refs[:1], refs[max(head, 1) :]
    ready_out, scale_out, refs = refs[0], refs[1], refs[2:]
    router, refs = (refs[0], refs[1:]) if routed else (None, refs)
    pay, notes, factors, turned, ready_factors, picks, ready, sem_in, sem_note, sem_out = refs
    chips, _, experts = notes.shape[1:4]
    half = experts // 2
    height = STEP * half
    steps = share // STEP
    outs = ready.shape[0]
    block = share * half

    def fetch(i):
        slot = lax.rem(i, depth)
        pltpu.make_async_copy(
            sources[0].at[:, :, rows_at(i * height, height, height), :], pay.at[slot], sem_in.at[slot]
        ).start()

    if head:
        core = lax.axis_index("core")
        for source, (dx, dy) in zip(sources, ((0, 0),) + SHIFTS):
            chip = chip_at(SIDE - dx, SIDE - dy)
            for k, which in enumerate((core, 1 - core)):
                pltpu.make_async_copy(
                    source.at[k, pl.ds(block, experts)], notes.at[0, chip, which], sem_note.at[0]
                ).start()
                pltpu.make_async_copy(source.at[k, pl.ds(0, block)], pay.at[0, chip, which], sem_in.at[0]).start()
    else:
        for k in range(1 + routed):
            rows = pl.ds(block + k * experts, experts)
            pltpu.make_async_copy(sources[0].at[:, :, rows, :], notes.at[k], sem_note.at[k]).start()

        def first(i, carry):
            fetch(i)
            return carry

        lax.fori_loop(0, depth, first, 0)

    copies = 3
    row = lax.broadcasted_iota(jnp.int32, (LANES, LANES), 0)
    right = jnp.where(lax.broadcasted_iota(jnp.int32, (LANES, LANES), 1) < HALF, 0, 1)
    peer = jnp.where(row < copies * 2 * chips, lax.rem(row, 2 * chips), -1)
    for q in range(chips):
        picks[:, q * LANES : (q + 1) * LANES] = jnp.where(peer == 2 * q + right, 1.0, 0.0).astype(jnp.bfloat16)

    def plain(code):
        y = code.astype(jnp.float32)
        size = jnp.maximum(jnp.abs(y), 1.2e-38)
        return y * jnp.exp2(jnp.log2(size) * (1.0 / POWER - 1.0))

    if routed:
        landed(notes.at[1], sem_note.at[1])
        for q in range(chips):
            a, b = (notes[1, q, c].astype(jnp.float32)[:half] for c in range(2))
            router[:, q * LANES : (q + 1) * LANES] = two_cores(a, b).astype(jnp.bfloat16)

    landed(notes.at[0], sem_note.at[0])
    part = notes[0].astype(jnp.float32).reshape(2 * chips, experts, LANES)
    part = part + pltpu.roll(part, HALF, 2)
    scale = jnp.sqrt(jnp.sum(part, 0))
    scale_out[...] = scale[:, :share]
    part = jnp.sqrt(jnp.maximum(part, FLOOR)) * (1.0 / (REACH * scale))[None]
    factors[...] = part.reshape(2 * chips * experts, LANES)
    tall = ready_factors.shape[0] // experts
    for e in range(experts):
        value = factors[pl.ds(e, 2 * chips, stride=experts), :]
        pieces = []
        for _ in range(copies):
            pieces.append(value.astype(jnp.bfloat16).astype(jnp.float32))
            value = value - pieces[-1]
        pieces.append(jnp.zeros((LANES - copies * 2 * chips, LANES), jnp.float32))
        turned[pl.ds(e, tall, stride=experts), :] = jnp.concatenate(pieces, 0).T[:tall]
    ready_factors[...] = turned[...].astype(jnp.bfloat16)
    if head:
        landed(pay, sem_in.at[0])

    def step_of(s, carry):
        out_slot = lax.rem(s, outs)
        if head:
            slot, base = 0, s * height
        else:
            slot, base = lax.rem(s, depth), 0
            landed(pay.at[slot], sem_in.at[slot])

        @pl.when(s >= outs)
        def _():
            landed(ready.at[out_slot], sem_out.at[out_slot])

        known = ready_factors[rows_at(s * STEP * experts, STEP * experts, STEP * experts), :]
        for q in range(chips):
            if q % 2 == 0:
                wide = picks[:, q * LANES : (q + 2) * LANES]
                factor = jnp.dot(known, wide, preferred_element_type=jnp.float32)
            mine = factor[:, q % 2 * LANES : (q % 2 + 1) * LANES]
            for p in range(STEP // 2):
                rows = rows_at(base + 2 * half * p, 2 * half, 2 * half)
                a2, b2 = (plain(pay[slot, q, c, rows, :]) for c in range(2))
                for h in range(2):
                    j = 2 * p + h
                    value = two_cores(a2[half * h : half * (h + 1)], b2[half * h : half * (h + 1)])
                    value = value * mine[experts * j : experts * (j + 1)]
                    ready[out_slot, j, :, q * LANES : (q + 1) * LANES] = value.astype(jnp.bfloat16)

        if not head:

            @pl.when(s + depth < steps)
            def _():
                fetch(s + depth)

        pltpu.make_async_copy(ready.at[out_slot], ready_out.at[pl.ds(s * STEP, STEP)], sem_out.at[out_slot]).start()
        return carry

    lax.fori_loop(0, steps, step_of, 0)
    for slot in range(outs):
        landed(ready.at[slot], sem_out.at[slot])


def decode(sources, experts, share, rows, routed, depth=8, outs=6):
    head = len(sources) if len(sources) > 1 else 0
    chips = head or sources[0].shape[0]
    half = experts // 2
    tall = -(-share // 8) * 8
    depth, high = (1, share * half) if head else (depth, STEP * half)
    vmem = pl.BlockSpec(memory_space=pltpu.VMEM)
    return pl.pallas_call(
        functools.partial(decode_kernel, share, depth, head, routed),
        in_specs=anywhere(len(sources)),
        out_specs=anywhere(1) + [vmem] * (1 + routed),
        out_shape=[
            jax.ShapeDtypeStruct((share, experts, rows * 2 * chips), jnp.bfloat16),
            jax.ShapeDtypeStruct((experts, share), jnp.float32),
        ]
        + [jax.ShapeDtypeStruct((experts, rows * 2 * chips), jnp.bfloat16)] * routed,
        scratch_shapes=[
            pltpu.VMEM((depth, chips, 2, high, LANES), jnp.bfloat16),
            pltpu.VMEM((1 + routed, chips, 2, experts, LANES), jnp.bfloat16),
            pltpu.VMEM((2 * chips * experts, LANES), jnp.float32),
            pltpu.VMEM((tall * experts, LANES), jnp.float32),
            pltpu.VMEM((tall * experts, LANES), jnp.bfloat16),
            pltpu.VMEM((LANES, chips * LANES), jnp.bfloat16),
            pltpu.VMEM((outs, STEP, experts, rows * 2 * chips), jnp.bfloat16),
            pltpu.SemaphoreType.DMA((depth,)),
            pltpu.SemaphoreType.DMA((1 + routed,)),
            pltpu.SemaphoreType.DMA((outs,)),
        ],
        name="decode_head" if head else "decode_bulk",
    )(*sources)


def moved(value, dx, dy):
    pairs = []
    for y in range(SIDE):
        for x in range(SIDE):
            to = (y + dy) % SIDE * SIDE + (x + dx) % SIDE
            pairs += [(2 * (y * SIDE + x) + core, 2 * to + core) for core in range(2)]
    return lax.ppermute(value, PLANE, pairs)


def body(train_gate, train_up, train_down, router_weight, router_gain):
    peers = lax.axis_size(PLANE)
    experts, rows, columns = train_gate.shape
    share = columns // peers

    def bulk_decoded(arrived, routed):
        return decode((arrived.reshape(peers // 2, 2, *arrived.shape[1:]),), experts, share, rows, routed)

    first = encode_bulk(train_up, (router_weight.T, router_gain[None]), (), peers)
    arrived_first = lax.all_to_all(first, PLANE, 0, 0, tiled=True)
    keep, give = encode_head(train_gate, (first,), peers)
    got = lax.ppermute(give, "core", ((0, 1), (1, 0)))
    second = encode_bulk(jnp.swapaxes(train_down, 1, 2), (), (keep,), peers)
    arrived = list(paired(keep, got))
    for k, shift in enumerate(SHIFTS):
        arrived[k + 1] = moved(arrived[k + 1], *shift)
    arrived_second = lax.all_to_all(second, PLANE, 0, 0, tiled=True)
    up, scale_up, router = bulk_decoded(arrived_first, 1)
    router = lax.all_gather(router, "ep", axis=0, tiled=True)
    gate, scale_gate = decode(tuple(arrived), experts, share, rows, 0)
    down, scale_down = bulk_decoded(arrived_second, 0)
    return (
        jnp.transpose(gate, (1, 2, 0)),
        jnp.transpose(up, (1, 2, 0)),
        jnp.transpose(down, (1, 0, 2)),
        scale_gate,
        scale_up,
        scale_down,
        router.T,
    )


def solution(mesh):
    fine = Mesh(mesh.devices.reshape(mesh.devices.shape[0], SIDE, SIDE, 2), ("ep",) + PLANE)
    return jax.shard_map(
        body,
        mesh=fine,
        in_specs=(
            P("ep", PLANE, None),
            P("ep", PLANE, None),
            P("ep", None, PLANE),
            P(PLANE, "ep"),
            P(PLANE),
        ),
        out_specs=(
            P("ep", None, PLANE),
            P("ep", None, PLANE),
            P("ep", PLANE, None),
            P("ep", PLANE),
            P("ep", PLANE),
            P("ep", PLANE),
            P(),
        ),
        check_vma=False,
    )
```

```python
import functools

import jax
import jax.numpy as jnp
from jax import lax
from jax.experimental import pallas as pl
from jax.experimental.pallas import tpu as pltpu
from jax.sharding import Mesh, PartitionSpec as P


POWER = 17
REACH = 180.0
FLOOR = 1e-37
LANES = 128
HALF = LANES // 2
STEP = 4
SIDE = 4
CHIPS = SIDE * SIDE
PLANE = ("y", "x", "core")
TURNS = (1, 3, 2)


def anywhere(count):
    return [pl.BlockSpec(memory_space=pl.ANY)] * count


def rows_at(start, size, unit):
    return pl.ds(pl.multiple_of(start, unit), size)


def landed(ref, sem):
    pltpu.make_async_copy(ref, ref, sem).wait()


def chip_at(dx, dy):
    y, x = lax.axis_index("y"), lax.axis_index("x")
    return lax.rem(y + dy, SIDE) * SIDE + lax.rem(x + dx, SIDE)


def behind(ahead, kernel):
    return lambda *refs: kernel(*refs[ahead:])


def encode_tiles(x, xin, stage, pay, sums, notes, sem_in, peers, tiles, after):
    depth, experts, _, _ = xin.shape
    half = experts // 2
    share = tiles * LANES // peers
    odd = lax.axis_index("core")

    def fetch(i):
        slot = lax.rem(i, depth)
        at = rows_at(i * LANES, LANES, LANES)
        pltpu.make_async_copy(x.at[:, :, at], xin.at[slot], sem_in.at[slot]).start()

    def first(i, carry):
        fetch(i)
        return carry

    lax.fori_loop(0, depth, first, 0)

    def tile_of(i, carry):
        slot = lax.rem(i, depth)
        landed(xin.at[slot], sem_in.at[slot])
        at = rows_at(i * LANES, LANES, LANES)
        for e in range(half):
            a, b = xin[slot, e + half * odd], xin[slot, e + half * (1 - odd)]
            sa = jnp.sum(a * a, 0, keepdims=True)
            sb = jnp.sum(b * b, 0, keepdims=True)
            sums[pl.ds(e, 1), at] = sa
            sums[pl.ds(e + half, 1), at] = sb
            a = a * (REACH * lax.rsqrt(jnp.maximum(sa, FLOOR)))
            b = b * (REACH * lax.rsqrt(jnp.maximum(sb, FLOOR)))
            v = jnp.concatenate([a, b], 0)
            v2 = v * v
            v4 = v2 * v2
            v8 = v4 * v4
            y = v8 * v8 * v
            stage[pl.ds(e, LANES, stride=half), :] = y.T
        pay[rows_at(i * LANES * half, LANES * half, LANES * half), :] = stage[...].astype(jnp.bfloat16)

        @pl.when(i + depth < tiles)
        def _():
            fetch(i + depth)

        after(i)
        return carry

    lax.fori_loop(0, tiles, tile_of, 0)
    total = sums[...]
    total = jnp.where(odd == 1, jnp.concatenate([total[half:], total[:half]], 0), total)
    high = total.astype(jnp.bfloat16).astype(jnp.float32)
    low = total - high
    gap = jnp.zeros((experts, HALF - share), jnp.float32)
    for d in range(peers):
        piece = slice(d * share, (d + 1) * share)
        notes[d] = jnp.concatenate([high[:, piece], gap, low[:, piece], gap], 1).astype(jnp.bfloat16)


def encode_scratch(peers, experts, rows, columns, depth):
    return [
        pltpu.VMEM((depth, experts, rows, LANES), jnp.float32),
        pltpu.VMEM((LANES * experts // 2, LANES), jnp.float32),
        pltpu.VMEM((columns * experts // 2, LANES), jnp.bfloat16),
        pltpu.VMEM((experts, columns), jnp.float32),
        pltpu.VMEM((peers, experts, LANES), jnp.bfloat16),
        pltpu.SemaphoreType.DMA((depth,)),
        pltpu.SemaphoreType.DMA,
        pltpu.SemaphoreType.DMA,
    ]


def encode_bulk_kernel(routed, peers, tiles, *refs):
    x, out = refs[0], refs[1 + 2 * routed]
    xin, stage, pay, sums, notes, sem_in, sem_pay, sem_note = refs[2 + 2 * routed : 10 + 2 * routed]
    experts = xin.shape[1]
    half = experts // 2
    share = tiles * LANES // peers
    block = share * half

    if routed:
        weight, gain = refs[1:3]
        router, sem_router = refs[10 + 2 * routed :]
        part = weight[...] * gain[...]
        part = jnp.where(lax.axis_index("core") == 1, jnp.concatenate([part[half:], part[:half]], 0), part)
        part = jnp.concatenate([part[:half], part[half:]], 1)
        part = jnp.concatenate([part, jnp.zeros_like(part)], 0).astype(jnp.bfloat16)
        for d in range(peers):
            router[d] = part
        pltpu.make_async_copy(router, out.at[:, pl.ds(block + experts, experts), :], sem_router).start()

    def after(tile):
        def send(d, inner):
            pltpu.make_async_copy(
                pay.at[rows_at(d * block, block, 16), :], out.at[d, pl.ds(0, block), :], sem_pay
            ).start()
            return inner

        lax.fori_loop(tile * LANES // share, (tile + 1) * LANES // share, send, 0)

    encode_tiles(x, xin, stage, pay, sums, notes, sem_in, peers, tiles, after)
    pltpu.make_async_copy(notes, out.at[:, pl.ds(block, experts), :], sem_note).start()
    landed(pay, sem_pay)
    landed(notes, sem_note)
    if routed:
        landed(router, sem_router)


def encode_bulk(x, small, ahead, peers, depth=8):
    experts, rows, columns = x.shape
    routed = len(small) // 2
    height = columns // peers * experts // 2 + experts * (1 + routed)
    return pl.pallas_call(
        behind(len(ahead), functools.partial(encode_bulk_kernel, routed, peers, columns // LANES)),
        in_specs=anywhere(len(ahead) + 1) + [pl.BlockSpec(memory_space=pltpu.VMEM)] * len(small),
        out_specs=pl.BlockSpec(memory_space=pl.ANY),
        out_shape=jax.ShapeDtypeStruct((peers, height, LANES), jnp.bfloat16),
        scratch_shapes=encode_scratch(peers, experts, rows, columns, depth)
        + [pltpu.VMEM((peers, experts, LANES), jnp.bfloat16), pltpu.SemaphoreType.DMA] * routed,
        name="encode_bulk",
    )(*ahead, x, *small)


def encode_head_kernel(peers, tiles, cut, x, *refs):
    by_x, by_y, scratch = refs[:SIDE], refs[SIDE : 2 * SIDE], refs[2 * SIDE :]
    xin, stage, pay, sums, notes, sem_in, sem_pay, sem_note = scratch
    experts = xin.shape[1]
    block = tiles * LANES // peers * experts // 2
    encode_tiles(x, xin, stage, pay, sums, notes, sem_in, peers, tiles, lambda tile: None)
    for dx in range(SIDE):
        for dy in range(SIDE):
            for core in range(2):
                d = 2 * chip_at(dx, dy) + core
                for out, start, size in (
                    (by_x[dx].at[core, dy], 0, cut),
                    (by_y[dy].at[core, dx, pl.ds(0, block - cut)], cut, block - cut),
                ):
                    pltpu.make_async_copy(pay.at[rows_at(d * block + start, size, 16), :], out, sem_pay).start()
                out = by_y[dy].at[core, dx, pl.ds(block - cut, experts)]
                pltpu.make_async_copy(notes.at[d], out, sem_note).start()
    landed(pay, sem_pay)
    landed(notes, sem_note)


def encode_head(x, cut, ahead, peers, depth=8):
    experts, rows, columns = x.shape
    height = columns // peers * experts // 2 + experts
    return pl.pallas_call(
        behind(len(ahead), functools.partial(encode_head_kernel, peers, columns // LANES, cut)),
        in_specs=anywhere(len(ahead) + 1),
        out_specs=anywhere(2 * SIDE),
        out_shape=[
            jax.ShapeDtypeStruct((2, SIDE, size, LANES), jnp.bfloat16)
            for size in (cut, height - cut)
            for _ in range(SIDE)
        ],
        scratch_shapes=encode_scratch(peers, experts, rows, columns, depth),
        name="encode_head",
    )(*ahead, x)


def sift_kernel(*refs):
    ins, give, (held_x, held_y, sem_in, sem_out) = refs[: 2 * SIDE], refs[2 * SIDE], refs[2 * SIDE + 1 :]
    other = 1 - lax.axis_index("core")
    cut, rest = held_x.shape[2], held_y.shape[2]
    for g, held in enumerate((held_x, held_y)):
        for i in range(SIDE):
            pltpu.make_async_copy(ins[SIDE * g + i].at[other], held.at[i], sem_in.at[g]).start()
    landed(held_x, sem_in.at[0])
    for i in range(SIDE):
        pltpu.make_async_copy(held_x.at[i], give.at[i, :, pl.ds(0, cut)], sem_out.at[0]).start()
    landed(held_y, sem_in.at[1])
    for i in range(SIDE):
        pltpu.make_async_copy(held_y.at[i], give.at[i, :, pl.ds(cut, rest)], sem_out.at[1]).start()
    landed(held_x, sem_out.at[0])
    landed(held_y, sem_out.at[1])


def sifted(arrays):
    cut, rest = arrays[0].shape[2], arrays[SIDE].shape[2]
    return pl.pallas_call(
        sift_kernel,
        in_specs=anywhere(2 * SIDE),
        out_specs=pl.BlockSpec(memory_space=pl.ANY),
        out_shape=jax.ShapeDtypeStruct((SIDE, SIDE, cut + rest, LANES), jnp.bfloat16),
        scratch_shapes=[pltpu.VMEM((SIDE, SIDE, size, LANES), jnp.bfloat16) for size in (cut, rest)]
        + [pltpu.SemaphoreType.DMA((2,)), pltpu.SemaphoreType.DMA((2,))],
        name="sifted",
    )(*arrays)


def cross_kernel(got, *refs):
    ins, outs, (held_x, held_y, sem_in, sem_out) = refs[:8], refs[8:16], refs[16:]
    core = lax.axis_index("core")
    start = 0
    for g, held in enumerate((held_x, held_y)):
        size = held.shape[3]
        for i in range(SIDE):
            pltpu.make_async_copy(ins[SIDE * g + i].at[core], held.at[0, i], sem_in.at[g]).start()
            pltpu.make_async_copy(got.at[i, :, pl.ds(start, size)], held.at[1, i], sem_in.at[g]).start()
        start += size
    for g, held in enumerate((held_x, held_y)):
        landed(held, sem_in.at[g])
        for j in range(SIDE):
            pltpu.make_async_copy(held.at[:, :, j], outs[SIDE * g + j], sem_out.at[g]).start()
    for g, held in enumerate((held_x, held_y)):
        landed(held, sem_out.at[g])


def crossed(got, arrays):
    shapes = [a.shape for a in arrays]
    return pl.pallas_call(
        cross_kernel,
        in_specs=anywhere(1 + 2 * SIDE),
        out_specs=anywhere(2 * SIDE),
        out_shape=[jax.ShapeDtypeStruct(shape, jnp.bfloat16) for shape in shapes],
        scratch_shapes=[pltpu.VMEM((2, SIDE, *shapes[k][1:]), jnp.bfloat16) for k in (0, SIDE)]
        + [pltpu.SemaphoreType.DMA((2,)), pltpu.SemaphoreType.DMA((2,))],
        name="crossed",
    )(got, *arrays)


def two_cores(a, b):
    left = lax.broadcasted_iota(jnp.int32, a.shape, 1) < HALF
    return jnp.concatenate([jnp.where(left, a, b), pltpu.roll(jnp.where(left, b, a), HALF, 1)], 0)


def plain(code):
    y = code.astype(jnp.float32)
    size = jnp.maximum(jnp.abs(y), 1.2e-38)
    return y * jnp.exp2(jnp.log2(size) * (1.0 / POWER - 1.0))


COPIES = 3


def spread_picks(picks):
    row = lax.broadcasted_iota(jnp.int32, (LANES, LANES), 0)
    right = jnp.where(lax.broadcasted_iota(jnp.int32, (LANES, LANES), 1) < HALF, 0, 1)
    peer = jnp.where(row < COPIES * 2 * CHIPS, lax.rem(row, 2 * CHIPS), -1)
    for q in range(CHIPS):
        picks[:, q * LANES : (q + 1) * LANES] = jnp.where(peer == 2 * q + right, 1.0, 0.0).astype(jnp.bfloat16)


def factors_from(notes, scale_out, factors, turned, ready_factors):
    experts, share = scale_out.shape
    part = notes[...].astype(jnp.float32).reshape(2 * CHIPS, experts, LANES)
    part = part + pltpu.roll(part, HALF, 2)
    scale = jnp.sqrt(jnp.sum(part, 0))
    scale_out[...] = scale[:, :share]
    part = jnp.sqrt(jnp.maximum(part, FLOOR)) * (1.0 / (REACH * scale))[None]
    factors[...] = part.reshape(2 * CHIPS * experts, LANES)
    tall = ready_factors.shape[0] // experts
    for e in range(experts):
        value = factors[pl.ds(e, 2 * CHIPS, stride=experts), :]
        pieces = []
        for _ in range(COPIES):
            pieces.append(value.astype(jnp.bfloat16).astype(jnp.float32))
            value = value - pieces[-1]
        pieces.append(jnp.zeros((LANES - COPIES * 2 * CHIPS, LANES), jnp.float32))
        turned[pl.ds(e, tall, stride=experts), :] = jnp.concatenate(pieces, 0).T[:tall]
    ready_factors[...] = turned[...].astype(jnp.bfloat16)


def decode_step(s, ready_out, ready_factors, picks, ready, sem_out, load, place):
    outs, _, experts, _ = ready.shape
    half = experts // 2
    out_slot = lax.rem(s, outs)

    @pl.when(s >= outs)
    def _():
        landed(ready.at[out_slot], sem_out.at[out_slot])

    known = ready_factors[rows_at(s * STEP * experts, STEP * experts, STEP * experts), :]
    for q in range(CHIPS):
        if q % 2 == 0:
            wide = picks[:, q * LANES : (q + 2) * LANES]
            factor = jnp.dot(known, wide, preferred_element_type=jnp.float32)
        mine = factor[:, q % 2 * LANES : (q % 2 + 1) * LANES]
        for p in range(STEP // 2):
            a2, b2 = (plain(load(q, which, p)) for which in range(2))
            for h in range(2):
                j = 2 * p + h
                value = two_cores(a2[half * h : half * (h + 1)], b2[half * h : half * (h + 1)])
                value = value * mine[experts * j : experts * (j + 1)]
                ready[out_slot, j, :, rows_at(place(q) * LANES, LANES, LANES)] = value.astype(jnp.bfloat16)
    pltpu.make_async_copy(ready.at[out_slot], ready_out.at[pl.ds(s * STEP, STEP)], sem_out.at[out_slot]).start()


def decode_scratch(experts, share, rows, outs):
    tall = -(-share // 8) * 8
    return [
        pltpu.VMEM((2 * CHIPS * experts, LANES), jnp.float32),
        pltpu.VMEM((tall * experts, LANES), jnp.float32),
        pltpu.VMEM((tall * experts, LANES), jnp.bfloat16),
        pltpu.VMEM((LANES, CHIPS * LANES), jnp.bfloat16),
        pltpu.VMEM((outs, STEP, experts, rows * 2 * CHIPS), jnp.bfloat16),
        pltpu.SemaphoreType.DMA((outs,)),
    ]


def decoded_shapes(experts, share, rows):
    return [
        jax.ShapeDtypeStruct((share, experts, rows * 2 * CHIPS), jnp.bfloat16),
        jax.ShapeDtypeStruct((experts, share), jnp.float32),
    ]


def decode_bulk_kernel(depth, source, ready_out, scale_out, router, pay, notes, sem_in, sem_note, *scratch):
    factors, turned, ready_factors, picks, ready, sem_out = scratch
    experts, share = scale_out.shape
    half = experts // 2
    height = STEP * half
    steps = share // STEP

    def fetch(i):
        slot = lax.rem(i, depth)
        rows = rows_at(i * height, height, height)
        pltpu.make_async_copy(source.at[:, :, rows, :], pay.at[slot], sem_in.at[slot]).start()

    for k in range(2):
        rows = pl.ds(share * half + k * experts, experts)
        pltpu.make_async_copy(source.at[:, :, rows, :], notes.at[k], sem_note.at[k]).start()

    def first(i, carry):
        fetch(i)
        return carry

    lax.fori_loop(0, depth, first, 0)
    spread_picks(picks)
    landed(notes.at[1], sem_note.at[1])
    for q in range(CHIPS):
        a, b = (notes[1, q, c].astype(jnp.float32)[:half] for c in range(2))
        router[:, q * LANES : (q + 1) * LANES] = two_cores(a, b).astype(jnp.bfloat16)
    landed(notes.at[0], sem_note.at[0])
    factors_from(notes.at[0], scale_out, factors, turned, ready_factors)

    def step_of(s, carry):
        slot = lax.rem(s, depth)
        landed(pay.at[slot], sem_in.at[slot])

        def load(q, which, p):
            return pay[slot, q, which, 2 * half * p : 2 * half * (p + 1), :]

        decode_step(s, ready_out, ready_factors, picks, ready, sem_out, load, lambda q: q)

        @pl.when(s + depth < steps)
        def _():
            fetch(s + depth)

        return carry

    lax.fori_loop(0, steps, step_of, 0)
    for slot in range(ready.shape[0]):
        landed(ready.at[slot], sem_out.at[slot])


def decode_bulk(source, experts, share, rows, depth=8, outs=6):
    vmem = pl.BlockSpec(memory_space=pltpu.VMEM)
    return pl.pallas_call(
        functools.partial(decode_bulk_kernel, depth),
        in_specs=anywhere(1),
        out_specs=anywhere(1) + [vmem] * 2,
        out_shape=decoded_shapes(experts, share, rows)
        + [jax.ShapeDtypeStruct((experts, rows * 2 * CHIPS), jnp.bfloat16)],
        scratch_shapes=[
            pltpu.VMEM((depth, CHIPS, 2, STEP * experts // 2, LANES), jnp.bfloat16),
            pltpu.VMEM((2, CHIPS, 2, experts, LANES), jnp.bfloat16),
            pltpu.SemaphoreType.DMA((depth,)),
            pltpu.SemaphoreType.DMA((2,)),
        ]
        + decode_scratch(experts, share, rows, outs),
        name="decode_bulk",
    )(source)


def decode_head_kernel(*refs):
    by_x, by_y, refs = refs[:SIDE], refs[SIDE : 2 * SIDE], refs[2 * SIDE :]
    ready_out, scale_out, *refs = refs
    held_x, held_y, notes, sem_in, sem_note, factors, turned, ready_factors, picks, ready, sem_out = refs
    experts, share = scale_out.shape
    half = experts // 2
    height = STEP * half
    steps = share // STEP
    turn = held_x.shape[3] // height
    core = lax.axis_index("core")
    even = (core, 1 - core)

    for i in range(SIDE):
        rows = pl.ds((steps - turn) * height, experts)
        pltpu.make_async_copy(by_y[i].at[:, :, rows], held_y.at[i, :, :, rows], sem_note).start()
    for s in range(steps):
        arrays, held, at = (by_x, held_x, s) if s < turn else (by_y, held_y, s - turn)
        rows = pl.ds(at * height, height)
        for i in range(SIDE):
            pltpu.make_async_copy(arrays[i].at[:, :, rows], held.at[i, :, :, rows], sem_in.at[s]).start()
    spread_picks(picks)
    landed(notes, sem_note)
    for dx in range(SIDE):
        for dy in range(SIDE):
            for which in range(2):
                rows = pl.ds((steps - turn) * height, experts)
                notes[SIDE * dx + dy, which] = held_y[dx, even[which], dy, rows, :]
    factors_from(notes, scale_out, factors, turned, ready_factors)

    def place(q):
        return chip_at(SIDE - q // SIDE, SIDE - q % SIDE)

    def step_with(held, first):
        def step_of(s, carry):
            landed(held.at[:, :, :, pl.ds(0, height)], sem_in.at[s])

            def load(q, which, p):
                i, j = (q % SIDE, q // SIDE) if first == 0 else (q // SIDE, q % SIDE)
                rows = rows_at((s - first) * height + 2 * half * p, 2 * half, 2 * half)
                return held[i, even[which], j, rows, :]

            decode_step(s, ready_out, ready_factors, picks, ready, sem_out, load, place)
            return carry

        return step_of

    lax.fori_loop(0, turn, step_with(held_x, 0), 0)
    lax.fori_loop(turn, steps, step_with(held_y, turn), 0)
    for slot in range(ready.shape[0]):
        landed(ready.at[slot], sem_out.at[slot])


def decode_head(parts, experts, share, rows, outs=6):
    vmem = pl.BlockSpec(memory_space=pltpu.VMEM)
    return pl.pallas_call(
        decode_head_kernel,
        in_specs=anywhere(len(parts)),
        out_specs=anywhere(1) + [vmem],
        out_shape=decoded_shapes(experts, share, rows),
        scratch_shapes=[pltpu.VMEM((SIDE, *parts[k].shape), jnp.bfloat16) for k in (0, SIDE)]
        + [
            pltpu.VMEM((CHIPS, 2, experts, LANES), jnp.bfloat16),
            pltpu.SemaphoreType.DMA((share // STEP,)),
            pltpu.SemaphoreType.DMA,
        ]
        + decode_scratch(experts, share, rows, outs),
        name="decode_head",
    )(*parts)


def join_kernel(*refs):
    parts, out = refs[:-1], refs[-1]
    count = len(parts)
    for k, part in enumerate(parts):
        plane = lax.rem(lax.axis_index("ep") + count - k, count)
        out[rows_at(plane * part.shape[0], part.shape[0], part.shape[0]), :] = part[...]


def joined(parts):
    rows, columns = parts[0].shape
    vmem = pl.BlockSpec(memory_space=pltpu.VMEM)
    return pl.pallas_call(
        join_kernel,
        in_specs=[vmem] * len(parts),
        out_specs=vmem,
        out_shape=jax.ShapeDtypeStruct((len(parts) * rows, columns), parts[0].dtype),
        name="joined",
    )(*parts)


def moved(value, axis, shift):
    return lax.ppermute(value, axis, [(k, (k + shift) % SIDE) for k in range(SIDE)])


def body(train_gate, train_up, train_down, router_weight, router_gain):
    peers = lax.axis_size(PLANE)
    experts, rows, columns = train_gate.shape
    share = columns // peers

    cut = STEP * experts // 2 * 6

    def phase(parts, axes):
        parts = list(parts)
        for shift in TURNS:
            for g, axis in enumerate(axes):
                parts[SIDE * g + shift] = moved(parts[SIDE * g + shift], axis, shift)
        return parts

    def halfway(parts):
        give = sifted(parts)
        got = lax.ppermute(give, "core", ((0, 1), (1, 0)))
        return crossed(got, parts)

    gate = encode_head(train_gate, cut, (), peers)
    first = encode_bulk(train_up, (router_weight.T, router_gain[None]), (gate[0],), peers)
    gate = phase(gate, ("x", "y"))
    arrived = lax.all_to_all(first, PLANE, 0, 0, tiled=True)
    down = encode_head(jnp.swapaxes(train_down, 1, 2), cut, (first,), peers)
    down = phase(down, ("x", "y"))
    gate = phase(halfway(gate), ("y", "x"))
    arrived = arrived.reshape(CHIPS, 2, *arrived.shape[1:])
    up, scale_up, router = decode_bulk(arrived, experts, share, rows)
    down = phase(halfway(down), ("y", "x"))
    planes = [router]
    for k in range(1, lax.axis_size("ep")):
        planes.append(moved(router, "ep", k))
    router = joined(planes)
    gate, scale_gate = decode_head(gate, experts, share, rows)
    down, scale_down = decode_head(down, experts, share, rows)
    return (
        jnp.transpose(gate, (1, 2, 0)),
        jnp.transpose(up, (1, 2, 0)),
        jnp.transpose(down, (1, 0, 2)),
        scale_gate,
        scale_up,
        scale_down,
        router.T,
    )


def solution(mesh):
    fine = Mesh(mesh.devices.reshape(mesh.devices.shape[0], SIDE, SIDE, 2), ("ep",) + PLANE)


    return jax.shard_map(
        body,
        mesh=fine,
        in_specs=(
            P("ep", PLANE, None),
            P("ep", PLANE, None),
            P("ep", None, PLANE),
            P(PLANE, "ep"),
            P(PLANE),
        ),
        out_specs=(
            P("ep", None, PLANE),
            P("ep", None, PLANE),
            P("ep", PLANE, None),
            P("ep", PLANE),
            P("ep", PLANE),
            P("ep", PLANE),
            P(),
        ),
        check_vma=False,
    )
```

```python
import functools

import jax
import jax.numpy as jnp
from jax import lax
from jax.experimental import pallas as pl
from jax.experimental.pallas import tpu as pltpu
from jax.sharding import Mesh, PartitionSpec as P


POWER = 17
REACH = 180.0
FLOOR = 1e-37
LANES = 128
HALF = LANES // 2
STEP = 4
SIDE = 4
CHIPS = SIDE * SIDE
PLANE = ("y", "x", "core")
TURNS = (1, 3, 2)


def anywhere(count):
    return [pl.BlockSpec(memory_space=pl.ANY)] * count


def rows_at(start, size, unit):
    return pl.ds(pl.multiple_of(start, unit), size)


def landed(ref, sem):
    pltpu.make_async_copy(ref, ref, sem).wait()


def chip_at(dx, dy):
    y, x = lax.axis_index("y"), lax.axis_index("x")
    return lax.rem(y + dy, SIDE) * SIDE + lax.rem(x + dx, SIDE)


def behind(ahead, kernel):
    return lambda *refs: kernel(*refs[ahead:])


def encode_tiles(x, xin, stage, pay, sums, notes, sem_in, peers, tiles, after):
    depth, experts, _, _ = xin.shape
    half = experts // 2
    share = tiles * LANES // peers
    odd = lax.axis_index("core")

    def fetch(i):
        slot = lax.rem(i, depth)
        at = rows_at(i * LANES, LANES, LANES)
        pltpu.make_async_copy(x.at[:, :, at], xin.at[slot], sem_in.at[slot]).start()

    def first(i, carry):
        fetch(i)
        return carry

    lax.fori_loop(0, depth, first, 0)

    def coded(i, at_stage):
        slot = lax.rem(i, depth)
        at = rows_at(i * LANES, LANES, LANES)
        for e in range(half):
            a, b = xin[slot, e + half * odd], xin[slot, e + half * (1 - odd)]
            sa = jnp.sum(a * a, 0, keepdims=True)
            sb = jnp.sum(b * b, 0, keepdims=True)
            sums[pl.ds(e, 1), at] = sa
            sums[pl.ds(e + half, 1), at] = sb
            a = a * (REACH * lax.rsqrt(jnp.maximum(sa, FLOOR)))
            b = b * (REACH * lax.rsqrt(jnp.maximum(sb, FLOOR)))
            v = jnp.concatenate([a, b], 0)
            v2 = v * v
            v4 = v2 * v2
            v8 = v4 * v4
            y = v8 * v8 * v
            at_stage[pl.ds(e, LANES, stride=half), :] = y.T

    def several(i, stages):
        for k in range(len(stages)):
            slot = lax.rem(i + k, depth)
            landed(xin.at[slot], sem_in.at[slot])
        for k, at_stage in enumerate(stages):
            coded(i + k, at_stage)
        for k, at_stage in enumerate(stages):
            rows = rows_at((i + k) * LANES * half, LANES * half, LANES * half)
            pay[rows, :] = at_stage[...].astype(jnp.bfloat16)
        for k in range(len(stages)):

            @pl.when(i + k + depth < tiles)
            def _():
                fetch(i + k + depth)

            after(i + k)

    def pair_of(m, carry):
        several(2 * m, stage)
        return carry

    lax.fori_loop(0, tiles // 2, pair_of, 0)
    for i in range(tiles // 2 * 2, tiles):
        several(i, stage[:1])
    total = sums[...]
    total = jnp.where(odd == 1, jnp.concatenate([total[half:], total[:half]], 0), total)
    high = total.astype(jnp.bfloat16).astype(jnp.float32)
    low = total - high
    gap = jnp.zeros((experts, HALF - share), jnp.float32)
    for d in range(peers):
        piece = slice(d * share, (d + 1) * share)
        notes[d] = jnp.concatenate([high[:, piece], gap, low[:, piece], gap], 1).astype(jnp.bfloat16)


def encode_scratch(peers, experts, rows, columns, depth):
    return [
        pltpu.VMEM((depth, experts, rows, LANES), jnp.float32),
        [pltpu.VMEM((LANES * experts // 2, LANES), jnp.float32)] * 2,
        pltpu.VMEM((columns * experts // 2, LANES), jnp.bfloat16),
        pltpu.VMEM((experts, columns), jnp.float32),
        pltpu.VMEM((peers, experts, LANES), jnp.bfloat16),
        pltpu.SemaphoreType.DMA((depth,)),
        pltpu.SemaphoreType.DMA,
        pltpu.SemaphoreType.DMA,
    ]


def encode_bulk_kernel(routed, peers, tiles, *refs):
    x, out = refs[0], refs[1 + 2 * routed]
    xin, stage, pay, sums, notes, sem_in, sem_pay, sem_note = refs[2 + 2 * routed : 10 + 2 * routed]
    experts = xin.shape[1]
    half = experts // 2
    share = tiles * LANES // peers
    block = share * half

    if routed:
        router, sem_router, weight, gain, sem_small = refs[10 + 2 * routed :]
        for k, small in enumerate((weight, gain)):
            pltpu.make_async_copy(refs[1 + k], small, sem_small.at[k]).start()

    def add_router():
        for k, small in enumerate((weight, gain)):
            landed(small, sem_small.at[k])
        part = weight[...] * gain[...]
        part = jnp.where(lax.axis_index("core") == 1, jnp.concatenate([part[half:], part[:half]], 0), part)
        part = jnp.concatenate([part[:half], part[half:]], 1)
        part = jnp.concatenate([part, jnp.zeros_like(part)], 0).astype(jnp.bfloat16)
        for d in range(peers):
            router[d] = part
        pltpu.make_async_copy(router, out.at[:, pl.ds(block + experts, experts), :], sem_router).start()

    def after(tile):
        def send(d, inner):
            pltpu.make_async_copy(
                pay.at[rows_at(d * block, block, 16), :], out.at[d, pl.ds(0, block), :], sem_pay
            ).start()
            return inner

        lax.fori_loop(tile * LANES // share, (tile + 1) * LANES // share, send, 0)

    encode_tiles(x, xin, stage, pay, sums, notes, sem_in, peers, tiles, after)
    if routed:
        add_router()
    pltpu.make_async_copy(notes, out.at[:, pl.ds(block, experts), :], sem_note).start()
    landed(pay, sem_pay)
    landed(notes, sem_note)
    if routed:
        landed(router, sem_router)


def encode_bulk(x, small, ahead, peers, depth=8):
    experts, rows, columns = x.shape
    routed = len(small) // 2
    height = columns // peers * experts // 2 + experts * (1 + routed)
    return pl.pallas_call(
        behind(len(ahead), functools.partial(encode_bulk_kernel, routed, peers, columns // LANES)),
        in_specs=anywhere(len(ahead) + 1 + len(small)),
        out_specs=pl.BlockSpec(memory_space=pl.ANY),
        out_shape=jax.ShapeDtypeStruct((peers, height, LANES), jnp.bfloat16),
        scratch_shapes=encode_scratch(peers, experts, rows, columns, depth)
        + [pltpu.VMEM((peers, experts, LANES), jnp.bfloat16), pltpu.SemaphoreType.DMA] * routed
        + [pltpu.VMEM(a.shape, a.dtype) for a in small]
        + [pltpu.SemaphoreType.DMA((2,))] * routed,
        name="encode_bulk",
    )(*ahead, x, *small)


def encode_head_kernel(peers, tiles, cut, x, *refs):
    by_x, by_y, scratch = refs[:SIDE], refs[SIDE : 2 * SIDE], refs[2 * SIDE :]
    xin, stage, pay, sums, notes, sem_in, sem_pay, sem_note = scratch
    experts = xin.shape[1]
    block = tiles * LANES // peers * experts // 2
    encode_tiles(x, xin, stage, pay, sums, notes, sem_in, peers, tiles, lambda tile: None)
    for dx in range(SIDE):
        for dy in range(SIDE):
            for core in range(2):
                d = 2 * chip_at(dx, dy) + core
                for out, start, size in (
                    (by_x[dx].at[core, dy], 0, cut),
                    (by_y[dy].at[core, dx, pl.ds(0, block - cut)], cut, block - cut),
                ):
                    pltpu.make_async_copy(pay.at[rows_at(d * block + start, size, 16), :], out, sem_pay).start()
                out = by_y[dy].at[core, dx, pl.ds(block - cut, experts)]
                pltpu.make_async_copy(notes.at[d], out, sem_note).start()
    landed(pay, sem_pay)
    landed(notes, sem_note)


def encode_head(x, cut, ahead, peers, depth=8):
    experts, rows, columns = x.shape
    height = columns // peers * experts // 2 + experts
    return pl.pallas_call(
        behind(len(ahead), functools.partial(encode_head_kernel, peers, columns // LANES, cut)),
        in_specs=anywhere(len(ahead) + 1),
        out_specs=anywhere(2 * SIDE),
        out_shape=[
            jax.ShapeDtypeStruct((2, SIDE, size, LANES), jnp.bfloat16)
            for size in (cut, height - cut)
            for _ in range(SIDE)
        ],
        scratch_shapes=encode_scratch(peers, experts, rows, columns, depth),
        name="encode_head",
    )(*ahead, x)


def sift_kernel(*refs):
    ins, give, (held_x, held_y, sem_in, sem_out) = refs[: 2 * SIDE], refs[2 * SIDE], refs[2 * SIDE + 1 :]
    other = 1 - lax.axis_index("core")
    cut, rest = held_x.shape[2], held_y.shape[2]
    for g, held in enumerate((held_x, held_y)):
        for i in range(SIDE):
            pltpu.make_async_copy(ins[SIDE * g + i].at[other], held.at[i], sem_in.at[g]).start()
    landed(held_x, sem_in.at[0])
    for i in range(SIDE):
        pltpu.make_async_copy(held_x.at[i], give.at[i, :, pl.ds(0, cut)], sem_out.at[0]).start()
    landed(held_y, sem_in.at[1])
    for i in range(SIDE):
        pltpu.make_async_copy(held_y.at[i], give.at[i, :, pl.ds(cut, rest)], sem_out.at[1]).start()
    landed(held_x, sem_out.at[0])
    landed(held_y, sem_out.at[1])


def sifted(arrays):
    cut, rest = arrays[0].shape[2], arrays[SIDE].shape[2]
    return pl.pallas_call(
        sift_kernel,
        in_specs=anywhere(2 * SIDE),
        out_specs=pl.BlockSpec(memory_space=pl.ANY),
        out_shape=jax.ShapeDtypeStruct((SIDE, SIDE, cut + rest, LANES), jnp.bfloat16),
        scratch_shapes=[pltpu.VMEM((SIDE, SIDE, size, LANES), jnp.bfloat16) for size in (cut, rest)]
        + [pltpu.SemaphoreType.DMA((2,)), pltpu.SemaphoreType.DMA((2,))],
        name="sifted",
    )(*arrays)


def cross_kernel(got, *refs):
    ins, outs, (held_x, held_y, sem_in, sem_out) = refs[:8], refs[8:16], refs[16:]
    core = lax.axis_index("core")
    start = 0
    for g, held in enumerate((held_x, held_y)):
        size = held.shape[3]
        for i in range(SIDE):
            pltpu.make_async_copy(ins[SIDE * g + i].at[core], held.at[0, i], sem_in.at[g]).start()
            pltpu.make_async_copy(got.at[i, :, pl.ds(start, size)], held.at[1, i], sem_in.at[g]).start()
        start += size
    for g, held in enumerate((held_x, held_y)):
        landed(held, sem_in.at[g])
        for j in range(SIDE):
            pltpu.make_async_copy(held.at[:, :, j], outs[SIDE * g + j], sem_out.at[g]).start()
    for g, held in enumerate((held_x, held_y)):
        landed(held, sem_out.at[g])


def crossed(got, arrays):
    shapes = [a.shape for a in arrays]
    return pl.pallas_call(
        cross_kernel,
        in_specs=anywhere(1 + 2 * SIDE),
        out_specs=anywhere(2 * SIDE),
        out_shape=[jax.ShapeDtypeStruct(shape, jnp.bfloat16) for shape in shapes],
        scratch_shapes=[pltpu.VMEM((2, SIDE, *shapes[k][1:]), jnp.bfloat16) for k in (0, SIDE)]
        + [pltpu.SemaphoreType.DMA((2,)), pltpu.SemaphoreType.DMA((2,))],
        name="crossed",
    )(got, *arrays)


def two_cores(a, b):
    left = lax.broadcasted_iota(jnp.int32, a.shape, 1) < HALF
    return jnp.concatenate([jnp.where(left, a, b), pltpu.roll(jnp.where(left, b, a), HALF, 1)], 0)


def plain(code):
    y = code.astype(jnp.float32)
    size = jnp.maximum(jnp.abs(y), 1.2e-38)
    return y * jnp.exp2(jnp.log2(size) * (1.0 / POWER - 1.0))


COPIES = 3


def spread_picks(picks):
    row = lax.broadcasted_iota(jnp.int32, (LANES, LANES), 0)
    right = jnp.where(lax.broadcasted_iota(jnp.int32, (LANES, LANES), 1) < HALF, 0, 1)
    peer = jnp.where(row < COPIES * 2 * CHIPS, lax.rem(row, 2 * CHIPS), -1)
    for q in range(CHIPS):
        picks[:, q * LANES : (q + 1) * LANES] = jnp.where(peer == 2 * q + right, 1.0, 0.0).astype(jnp.bfloat16)


def factors_from(notes, scale_out, factors, turned, ready_factors):
    experts, share = scale_out.shape
    part = notes[...].astype(jnp.float32).reshape(2 * CHIPS, experts, LANES)
    part = part + pltpu.roll(part, HALF, 2)
    scale = jnp.sqrt(jnp.sum(part, 0))
    scale_out[...] = scale[:, :share]
    part = jnp.sqrt(jnp.maximum(part, FLOOR)) * (1.0 / (REACH * scale))[None]
    factors[...] = part.reshape(2 * CHIPS * experts, LANES)
    tall = ready_factors.shape[0] // experts
    for e in range(experts):
        value = factors[pl.ds(e, 2 * CHIPS, stride=experts), :]
        pieces = []
        for _ in range(COPIES):
            pieces.append(value.astype(jnp.bfloat16).astype(jnp.float32))
            value = value - pieces[-1]
        pieces.append(jnp.zeros((LANES - COPIES * 2 * CHIPS, LANES), jnp.float32))
        turned[pl.ds(e, tall, stride=experts), :] = jnp.concatenate(pieces, 0).T[:tall]
    ready_factors[...] = turned[...].astype(jnp.bfloat16)


def decode_step(s, ready_out, ready_factors, picks, ready, sem_out, load, place):
    outs, _, experts, _ = ready.shape
    half = experts // 2
    out_slot = lax.rem(s, outs)

    @pl.when(s >= outs)
    def _():
        landed(ready.at[out_slot], sem_out.at[out_slot])

    known = ready_factors[rows_at(s * STEP * experts, STEP * experts, STEP * experts), :]
    for q in range(CHIPS):
        if q % 2 == 0:
            wide = picks[:, q * LANES : (q + 2) * LANES]
            factor = jnp.dot(known, wide, preferred_element_type=jnp.float32)
        mine = factor[:, q % 2 * LANES : (q % 2 + 1) * LANES]
        for p in range(STEP // 2):
            a2, b2 = (plain(load(q, which, p)) for which in range(2))
            for h in range(2):
                j = 2 * p + h
                value = two_cores(a2[half * h : half * (h + 1)], b2[half * h : half * (h + 1)])
                value = value * mine[experts * j : experts * (j + 1)]
                ready[out_slot, j, :, rows_at(place(q) * LANES, LANES, LANES)] = value.astype(jnp.bfloat16)
    pltpu.make_async_copy(ready.at[out_slot], ready_out.at[pl.ds(s * STEP, STEP)], sem_out.at[out_slot]).start()


def decode_scratch(experts, share, rows, outs):
    tall = -(-share // 8) * 8
    return [
        pltpu.VMEM((2 * CHIPS * experts, LANES), jnp.float32),
        pltpu.VMEM((tall * experts, LANES), jnp.float32),
        pltpu.VMEM((tall * experts, LANES), jnp.bfloat16),
        pltpu.VMEM((LANES, CHIPS * LANES), jnp.bfloat16),
        pltpu.VMEM((outs, STEP, experts, rows * 2 * CHIPS), jnp.bfloat16),
        pltpu.SemaphoreType.DMA((outs,)),
    ]


def decoded_shapes(experts, share, rows):
    return [
        jax.ShapeDtypeStruct((share, experts, rows * 2 * CHIPS), jnp.bfloat16),
        jax.ShapeDtypeStruct((experts, share), jnp.float32),
    ]


def decode_bulk_kernel(depth, source, ready_out, scale_out, router, pay, notes, sem_in, sem_note, *scratch):
    factors, turned, ready_factors, picks, ready, sem_out = scratch
    experts, share = scale_out.shape
    half = experts // 2
    height = STEP * half
    steps = share // STEP

    def fetch(i):
        slot = lax.rem(i, depth)
        rows = rows_at(i * height, height, height)
        pltpu.make_async_copy(source.at[:, :, rows, :], pay.at[slot], sem_in.at[slot]).start()

    for k in range(2):
        rows = pl.ds(share * half + k * experts, experts)
        pltpu.make_async_copy(source.at[:, :, rows, :], notes.at[k], sem_note.at[k]).start()

    def first(i, carry):
        fetch(i)
        return carry

    lax.fori_loop(0, depth, first, 0)
    spread_picks(picks)
    landed(notes.at[1], sem_note.at[1])
    for q in range(CHIPS):
        a, b = (notes[1, q, c].astype(jnp.float32)[:half] for c in range(2))
        router[:, q * LANES : (q + 1) * LANES] = two_cores(a, b).astype(jnp.bfloat16)
    landed(notes.at[0], sem_note.at[0])
    factors_from(notes.at[0], scale_out, factors, turned, ready_factors)

    def step_of(s, carry):
        slot = lax.rem(s, depth)
        landed(pay.at[slot], sem_in.at[slot])

        def load(q, which, p):
            return pay[slot, q, which, 2 * half * p : 2 * half * (p + 1), :]

        decode_step(s, ready_out, ready_factors, picks, ready, sem_out, load, lambda q: q)

        @pl.when(s + depth < steps)
        def _():
            fetch(s + depth)

        return carry

    lax.fori_loop(0, steps, step_of, 0)
    for slot in range(ready.shape[0]):
        landed(ready.at[slot], sem_out.at[slot])


def decode_bulk(source, experts, share, rows, depth=8, outs=6):
    vmem = pl.BlockSpec(memory_space=pltpu.VMEM)
    return pl.pallas_call(
        functools.partial(decode_bulk_kernel, depth),
        in_specs=anywhere(1),
        out_specs=anywhere(1) + [vmem] * 2,
        out_shape=decoded_shapes(experts, share, rows)
        + [jax.ShapeDtypeStruct((experts, rows * 2 * CHIPS), jnp.bfloat16)],
        scratch_shapes=[
            pltpu.VMEM((depth, CHIPS, 2, STEP * experts // 2, LANES), jnp.bfloat16),
            pltpu.VMEM((2, CHIPS, 2, experts, LANES), jnp.bfloat16),
            pltpu.SemaphoreType.DMA((depth,)),
            pltpu.SemaphoreType.DMA((2,)),
        ]
        + decode_scratch(experts, share, rows, outs),
        name="decode_bulk",
    )(source)


def decode_head_kernel(*refs):
    by_x, by_y, refs = refs[:SIDE], refs[SIDE : 2 * SIDE], refs[2 * SIDE :]
    ready_out, scale_to, scale_out, sem_scale, *refs = refs
    held_x, held_y, notes, sem_in, sem_note, factors, turned, ready_factors, picks, ready, sem_out = refs
    experts, share = scale_out.shape
    half = experts // 2
    height = STEP * half
    steps = share // STEP
    turn = held_x.shape[3] // height
    core = lax.axis_index("core")
    even = (core, 1 - core)

    for i in range(SIDE):
        rows = pl.ds((steps - turn) * height, experts)
        pltpu.make_async_copy(by_y[i].at[:, :, rows], held_y.at[i, :, :, rows], sem_note).start()
    for s in range(steps):
        arrays, held, at = (by_x, held_x, s) if s < turn else (by_y, held_y, s - turn)
        rows = pl.ds(at * height, height)
        for i in range(SIDE):
            pltpu.make_async_copy(arrays[i].at[:, :, rows], held.at[i, :, :, rows], sem_in.at[s]).start()
    spread_picks(picks)
    landed(notes, sem_note)
    for dx in range(SIDE):
        for dy in range(SIDE):
            for which in range(2):
                rows = pl.ds((steps - turn) * height, experts)
                notes[SIDE * dx + dy, which] = held_y[dx, even[which], dy, rows, :]
    factors_from(notes, scale_out, factors, turned, ready_factors)
    pltpu.make_async_copy(scale_out, scale_to, sem_scale).start()

    def place(q):
        return chip_at(SIDE - q // SIDE, SIDE - q % SIDE)

    def step_with(held, first):
        def step_of(s, carry):
            landed(held.at[:, :, :, pl.ds(0, height)], sem_in.at[s])

            def load(q, which, p):
                i, j = (q % SIDE, q // SIDE) if first == 0 else (q // SIDE, q % SIDE)
                rows = rows_at((s - first) * height + 2 * half * p, 2 * half, 2 * half)
                return held[i, even[which], j, rows, :]

            decode_step(s, ready_out, ready_factors, picks, ready, sem_out, load, place)
            return carry

        return step_of

    lax.fori_loop(0, turn, step_with(held_x, 0), 0)
    lax.fori_loop(turn, steps, step_with(held_y, turn), 0)
    landed(scale_out, sem_scale)
    for slot in range(ready.shape[0]):
        landed(ready.at[slot], sem_out.at[slot])


def decode_head(parts, experts, share, rows, outs=6):
    return pl.pallas_call(
        decode_head_kernel,
        in_specs=anywhere(len(parts)),
        out_specs=anywhere(2),
        out_shape=decoded_shapes(experts, share, rows),
        scratch_shapes=[pltpu.VMEM((experts, share), jnp.float32), pltpu.SemaphoreType.DMA]
        + [pltpu.VMEM((SIDE, *parts[k].shape), jnp.bfloat16) for k in (0, SIDE)]
        + [
            pltpu.VMEM((CHIPS, 2, experts, LANES), jnp.bfloat16),
            pltpu.SemaphoreType.DMA((share // STEP,)),
            pltpu.SemaphoreType.DMA,
        ]
        + decode_scratch(experts, share, rows, outs),
        name="decode_head",
    )(*parts)


def join_kernel(*refs):
    parts, out = refs[:-1], refs[-1]
    count = len(parts)
    for k, part in enumerate(parts):
        plane = lax.rem(lax.axis_index("ep") + count - k, count)
        out[rows_at(plane * part.shape[0], part.shape[0], part.shape[0]), :] = part[...]


def joined(parts):
    rows, columns = parts[0].shape
    vmem = pl.BlockSpec(memory_space=pltpu.VMEM)
    return pl.pallas_call(
        join_kernel,
        in_specs=[vmem] * len(parts),
        out_specs=vmem,
        out_shape=jax.ShapeDtypeStruct((len(parts) * rows, columns), parts[0].dtype),
        name="joined",
    )(*parts)


def moved(value, axis, shift):
    return lax.ppermute(value, axis, [(k, (k + shift) % SIDE) for k in range(SIDE)])


def body(train_gate, train_up, train_down, router_weight, router_gain):
    peers = lax.axis_size(PLANE)
    experts, rows, columns = train_gate.shape
    share = columns // peers

    cut = STEP * experts // 2 * 6

    def phase(parts, axes):
        parts = list(parts)
        for shift in TURNS:
            for g, axis in enumerate(axes):
                parts[SIDE * g + shift] = moved(parts[SIDE * g + shift], axis, shift)
        return parts

    def halfway(parts):
        give = sifted(parts)
        got = lax.ppermute(give, "core", ((0, 1), (1, 0)))
        return crossed(got, parts)

    gate = encode_head(train_gate, cut, (), peers)
    first = encode_bulk(train_up, (router_weight.T, router_gain[None]), (gate[0],), peers)
    gate = phase(gate, ("x", "y"))
    arrived = lax.all_to_all(first, PLANE, 0, 0, tiled=True)
    down = encode_head(jnp.swapaxes(train_down, 1, 2), cut, (first,), peers)
    down = phase(down, ("x", "y"))
    gate = phase(halfway(gate), ("y", "x"))
    arrived = arrived.reshape(CHIPS, 2, *arrived.shape[1:])
    up, scale_up, router = decode_bulk(arrived, experts, share, rows)
    down = phase(halfway(down), ("y", "x"))
    planes = [router]
    for k in range(1, lax.axis_size("ep")):
        planes.append(moved(router, "ep", k))
    router = joined(planes)
    gate, scale_gate = decode_head(gate, experts, share, rows)
    down, scale_down = decode_head(down, experts, share, rows)
    return (
        jnp.transpose(gate, (1, 2, 0)),
        jnp.transpose(up, (1, 2, 0)),
        jnp.transpose(down, (1, 0, 2)),
        scale_gate,
        scale_up,
        scale_down,
        router.T,
    )


def solution(mesh):
    fine = Mesh(mesh.devices.reshape(mesh.devices.shape[0], SIDE, SIDE, 2), ("ep",) + PLANE)


    return jax.shard_map(
        body,
        mesh=fine,
        in_specs=(
            P("ep", PLANE, None),
            P("ep", PLANE, None),
            P("ep", None, PLANE),
            P(PLANE, "ep"),
            P(PLANE),
        ),
        out_specs=(
            P("ep", None, PLANE),
            P("ep", None, PLANE),
            P("ep", PLANE, None),
            P("ep", PLANE),
            P("ep", PLANE),
            P("ep", PLANE),
            P(),
        ),
        check_vma=False,
    )
```
